32 devices in a mesh: rows: 8 (over z, x), width: 4 (over y, core).
Axes of the slice: x: 2, y: 2, z: 4, core: 2. Of those that a mesh axis runs over, the one named last changes fastest.
Arguments:
- w_gate: float32 [3072, 8192], P('rows', 'width'), may hold values from -0.15625 to 0.15625
- avg_gate: float32 [3072, 8192], P('rows', 'width'), may hold values from -0.109375 to 0.109375
- w_up: float32 [3072, 8192], P('rows', 'width'), may hold values from -0.15625 to 0.15625
- avg_up: float32 [3072, 8192], P('rows', 'width'), may hold values from -0.109375 to 0.109375
- norm_gain: float32 [3072], P('rows'), may hold values from 0.25 to 1.75
Outputs:
- serve_gate: bfloat16 [3072, 8192], P(None, 'width')
- serve_up: bfloat16 [3072, 8192], P(None, 'width')
- factor_gate: float32 [8192], P('width')
- factor_up: float32 [8192], P('width')
The draws below stay inside these ranges and needn't reach their ends.
All inputs are finite; a program needn't handle non-finite values. Where the reference program divides by a largest or mean magnitude, that divisor is 1e-20 or more.
Results may differ from the reference program's by a relative error of at most 0.001.
Values may be sent and summed in bfloat16 or wider, within the bound.
A program may use at most 128 MiB of HBM per device.

```python
import jax
import jax.numpy as jnp

D_MODEL = 3072
D_INNER = 8192


def with_spikes(drawn, rng, source, target, parts, factor):
    owner, partner = [(jnp.arange(drawn.shape[axis_at]) // (drawn.shape[axis_at] // parts)).reshape([-1 if axis == axis_at else 1 for axis in range(drawn.ndim)]) for axis_at in (source, target)]
    chosen = jax.random.permutation(rng, parts)[partner]
    strong = (owner == chosen) | (owner == (partner + parts // 2) % parts)
    return jnp.where(strong, factor * drawn, drawn)


def block_scale(stream_key, extent, shards, low, top_value):
    factor_of, own = 1.0, jax.random.fold_in(stream_key, 6)
    for axis_at, shards_of in shards:
        draws = jnp.exp(jax.random.uniform(jax.random.fold_in(own, axis_at), (shards_of,), jnp.float32, low / len(shards), top_value / len(shards)))
        factor_of = factor_of * jnp.repeat(draws, extent[axis_at] // shards_of).reshape([-1 if axis == axis_at else 1 for axis in range(len(extent))])
    return factor_of


def bell_draw(rng, shape, width, limit, split=(), kind=jnp.bfloat16):
    result = jax.random.normal(rng, shape, jnp.float32) * width
    if len(split) > 0:
        result = block_scale(rng, shape, split, -0.22, 0.18) * result
    return jnp.clip(result, min=-limit, max=limit).astype(kind)


def bell_draw_with(stream_key, extent, spread, reach, pieces, heavy, held_as=jnp.bfloat16):
    values = spread * jax.random.normal(stream_key, extent, jnp.float32)
    if pieces:
        values = values * block_scale(stream_key, extent, pieces, -0.22, 0.18)
    return jnp.clip(with_spikes(values, jax.random.fold_in(stream_key, 3), *heavy), -reach, reach).astype(held_as)


def setup_inputs(seed: int = 0) -> dict:
    keys = jax.random.split(jax.random.key(seed), 6)
    return {
        "w_gate": bell_draw_with(keys[0], (D_MODEL, D_INNER), D_MODEL ** -0.5, 0.15625, ((0, 8), (1, 4)), (0, 1, 8, 2.0), jnp.float32),
        "avg_gate": bell_draw(keys[1], (D_MODEL, D_INNER), D_MODEL ** -0.5, 0.109375, ((0, 8), (1, 4)), jnp.float32),
        "w_up": bell_draw_with(keys[2], (D_MODEL, D_INNER), D_MODEL ** -0.5, 0.15625, ((0, 8), (1, 4)), (0, 1, 8, 2.0), jnp.float32),
        "avg_up": bell_draw(keys[3], (D_MODEL, D_INNER), D_MODEL ** -0.5, 0.109375, ((0, 8), (1, 4)), jnp.float32),
        "norm_gain": jnp.clip(1.0 + 0.15 * jax.random.normal(keys[4], (D_MODEL,), jnp.float32), 0.25, 1.75),
    }


keep_rate = 0.7


def reference(w_gate, avg_gate, w_up, avg_up, norm_gain):
    fresh_gate = keep_rate * avg_gate + (1.0 - keep_rate) * w_gate
    fresh_up = keep_rate * avg_up + (1.0 - keep_rate) * w_up
    fresh_gained_gate = fresh_gate * norm_gain[:, None]
    fresh_gained_up = fresh_up * norm_gain[:, None]
    factor_gate = jnp.max(jnp.abs(fresh_gained_gate), axis=0)
    serve_gate = (fresh_gained_gate / factor_gate).astype(jnp.bfloat16)
    factor_up = jnp.max(jnp.abs(fresh_gained_up), axis=0)
    serve_up = (fresh_gained_up / factor_up).astype(jnp.bfloat16)
    return serve_gate, serve_up, factor_gate, factor_up
```

```python
import functools

import jax
import jax.numpy as jnp
from jax import lax
from jax.experimental import pallas as pl
from jax.experimental.pallas import tpu as pltpu
from jax.sharding import PartitionSpec as P

keep_rate = 0.7
MESH = pl.DeviceIdType.MESH
CHUNKS = 4


def ring_place(r, n):
    if n % 2:
        return r
    x, z = r % 2, r // 2
    return z + x * (n - 1 - 2 * z)


def ring_row(p, n):
    if n % 2:
        return p
    half = n // 2
    x, k = p // half, p % half
    return 2 * (k + x * (half - 1 - 2 * k)) + x


def maxima_kernel(n, part_ref, out_ref, got, send_sem, recv_sem):
    me = lax.axis_index("rows")
    barrier = pltpu.get_barrier_semaphore()
    for d in range(1, n):
        pl.semaphore_signal(barrier, inc=1, device_id={"rows": (me + d) % n}, device_id_type=MESH)
    pl.semaphore_wait(barrier, n - 1)
    copies = []
    for d in range(1, n):
        copy = pltpu.make_async_remote_copy(
            src_ref=part_ref,
            dst_ref=got.at[d - 1],
            send_sem=send_sem.at[d - 1],
            recv_sem=recv_sem.at[d - 1],
            device_id={"rows": (me + d) % n},
            device_id_type=MESH,
        )
        copy.start()
        copies.append(copy)
    for copy in copies:
        copy.wait()
    out_ref[...] = jnp.maximum(part_ref[...], jnp.max(got[...], axis=0))


def maxima(part, n):
    return pl.pallas_call(
        functools.partial(maxima_kernel, n),
        out_shape=jax.ShapeDtypeStruct(part.shape, part.dtype),
        in_specs=[pl.BlockSpec(memory_space=pltpu.VMEM)],
        out_specs=pl.BlockSpec(memory_space=pltpu.VMEM),
        scratch_shapes=[
            pltpu.VMEM((n - 1,) + part.shape, part.dtype),
            pltpu.SemaphoreType.DMA((n - 1,)),
            pltpu.SemaphoreType.DMA((n - 1,)),
        ],
        compiler_params=pltpu.CompilerParams(collective_id=0, has_side_effects=True),
        name="maxima",
    )(part)


def ring_kernel(n, chunks, a_ref, b_ref, ao_ref, bo_ref, send_sem, recv_sem, own_sem):
    me = lax.axis_index("rows")
    place = ring_place(me, n)
    nxt = ring_row((place + 1) % n, n)
    prv = ring_row((place + n - 1) % n, n)
    rows = a_ref.shape[0]
    size = rows // chunks

    barrier = pltpu.get_barrier_semaphore()
    for other in (nxt, prv):
        pl.semaphore_signal(barrier, inc=1, device_id={"rows": other}, device_id_type=MESH)
    pl.semaphore_wait(barrier, 2)

    def here(owner, c):
        return pl.ds(pl.multiple_of(owner * rows + c * size, size), size)

    def send(way, step, c, first):
        src, out, to = ((a_ref, ao_ref, nxt), (b_ref, bo_ref, prv))[way]
        turn = (n - step) if way == 0 else step
        at = here(ring_row((place + turn) % n, n), c)
        return pltpu.make_async_remote_copy(
            src_ref=src.at[pl.ds(c * size, size)] if first else out.at[at],
            dst_ref=out.at[at],
            send_sem=send_sem.at[way, step, c],
            recv_sem=recv_sem.at[way, step, c],
            device_id={"rows": to},
            device_id_type=MESH,
        )

    for c in range(chunks):
        for way in range(2):
            send(way, 0, c, True).start()
    own = [
        pltpu.make_async_copy(src, out.at[pl.ds(pl.multiple_of(me * rows, rows), rows)], own_sem.at[way])
        for way, (src, out) in enumerate(((a_ref, ao_ref), (b_ref, bo_ref)))
    ]
    for copy in own:
        copy.start()

    def landed(way, step, c):
        src, out, to = ((a_ref, ao_ref, nxt), (b_ref, bo_ref, prv))[way]
        turn = (n - step - 1) if way == 0 else (step + 1)
        at = here(ring_row((place + turn) % n, n), c)
        pltpu.make_async_remote_copy(
            src_ref=out.at[at],
            dst_ref=out.at[at],
            send_sem=send_sem.at[way, step, c],
            recv_sem=recv_sem.at[way, step, c],
            device_id={"rows": to},
            device_id_type=MESH,
        ).wait_recv()

    @pl.loop(1, n - 1)
    def _(step):
        for c in range(chunks):
            for way in range(2):
                landed(way, step - 1, c)
                send(way, step, c, False).start()

    for c in range(chunks):
        for way in range(2):
            landed(way, n - 2, c)
    for copy in own:
        copy.wait()
    for c in range(chunks):
        for way in range(2):
            send(way, 0, c, True).wait_send()

    @pl.loop(1, n - 1)
    def _(step):
        for c in range(chunks):
            for way in range(2):
                send(way, step, c, False).wait_send()


def ring(a, b, n):
    rows, columns = a.shape
    chunks = CHUNKS
    while rows % (16 * chunks):
        chunks -= 1
    whole = jax.ShapeDtypeStruct((n * rows, columns), a.dtype)
    return pl.pallas_call(
        functools.partial(ring_kernel, n, chunks),
        out_shape=(whole, whole),
        in_specs=[pl.BlockSpec(memory_space=pltpu.VMEM)] * 2,
        out_specs=(pl.BlockSpec(memory_space=pl.ANY), pl.BlockSpec(memory_space=pl.ANY)),
        scratch_shapes=[
            pltpu.SemaphoreType.DMA((2, n - 1, chunks)),
            pltpu.SemaphoreType.DMA((2, n - 1, chunks)),
            pltpu.SemaphoreType.DMA((2,)),
        ],
        compiler_params=pltpu.CompilerParams(collective_id=1, has_side_effects=True),
        name="ring",
    )(a, b)


def local(n, w_gate, avg_gate, w_up, avg_up, norm_gain):
    gain = norm_gain[:, None]

    def fresh(avg, w):
        return (keep_rate * avg + (1.0 - keep_rate) * w) * gain

    part = jnp.stack([jnp.max(jnp.abs(fresh(avg, w)), axis=0) for avg, w in ((avg_gate, w_gate), (avg_up, w_up))])
    factor = maxima(part, n)
    narrow_gate = (fresh(avg_gate, w_gate) / factor[0]).astype(jnp.bfloat16)
    narrow_up = (fresh(avg_up, w_up) / factor[1]).astype(jnp.bfloat16)
    serve_gate, serve_up = ring(narrow_gate, narrow_up, n)
    return (serve_gate, serve_up, factor[0], factor[1])


def solution(mesh):
    placed = (P("rows", "width"),) * 4 + (P("rows"),)
    return jax.shard_map(
        functools.partial(local, mesh.shape["rows"]),
        mesh=mesh,
        in_specs=placed,
        out_specs=(P(None, "width"), P(None, "width"), P("width"), P("width")),
        check_vma=False,
    )
```

```python
import functools

import jax
import jax.numpy as jnp
from jax import lax
from jax.experimental import pallas as pl
from jax.experimental.pallas import tpu as pltpu
from jax.sharding import PartitionSpec as P

keep_rate = 0.7
MESH = pl.DeviceIdType.MESH
CHUNKS = 4
VMEM_LIMIT = 60 * 2**20


def ring_place(r, n):
    if n % 2:
        return r
    x, z = r % 2, r // 2
    return z + x * (n - 1 - 2 * z)


def ring_row(p, n):
    if n % 2:
        return p
    half = n // 2
    x, k = p // half, p % half
    return 2 * (k + x * (half - 1 - 2 * k)) + x


def serve_kernel(
    n, chunks, gain_ref, wg_ref, ag_ref, wu_ref, au_ref, go_ref, uo_ref, fg_ref, fu_ref,
    w_in, fresh, narrow, part, got, in_sem, max_send, max_recv, send_sem, recv_sem, own_sem,
):
    me = lax.axis_index("rows")
    place = ring_place(me, n)
    nxt = ring_row((place + 1) % n, n)
    prv = ring_row((place + n - 1) % n, n)
    rows, columns = wg_ref.shape
    size = rows // chunks
    outs, to = (go_ref, uo_ref), (nxt, prv)

    loads = []
    for c in range(chunks):
        at = pl.ds(c * size, size)
        for k, (w_ref, avg_ref) in enumerate(((wg_ref, ag_ref), (wu_ref, au_ref))):
            for j, (src, dst) in enumerate(((w_ref, w_in), (avg_ref, fresh))):
                load = pltpu.make_async_copy(src.at[at], dst.at[k, at], in_sem.at[c, k, j])
                load.start()
                loads.append(load)

    barrier = pltpu.get_barrier_semaphore()
    for d in range(1, n):
        pl.semaphore_signal(barrier, inc=1, device_id={"rows": (me + d) % n}, device_id_type=MESH)

    tops = [jnp.zeros((8, columns), jnp.float32)] * 2
    for c in range(chunks):
        for k in range(2):
            loads[(c * 2 + k) * 2].wait()
            loads[(c * 2 + k) * 2 + 1].wait()

            def blend(i, top):
                at = pl.ds(pl.multiple_of(c * size + i * 8, 8), 8)
                gain = jnp.tile(gain_ref[at, :], (1, columns // 128))
                value = (keep_rate * fresh[k, at, :] + (1.0 - keep_rate) * w_in[k, at, :]) * gain
                fresh[k, at, :] = value
                return jnp.maximum(top, jnp.abs(value))

            tops[k] = lax.fori_loop(0, size // 8, blend, tops[k])
    for k in range(2):
        part[k : k + 1, :] = jnp.max(tops[k], axis=0, keepdims=True)

    pl.semaphore_wait(barrier, n - 1)
    copies = []
    for d in range(1, n):
        copy = pltpu.make_async_remote_copy(
            src_ref=part,
            dst_ref=got.at[d - 1],
            send_sem=max_send.at[d - 1],
            recv_sem=max_recv.at[d - 1],
            device_id={"rows": (me + d) % n},
            device_id_type=MESH,
        )
        copy.start()
        copies.append(copy)
    for copy in copies:
        copy.wait()
    factor = jnp.maximum(part[...], jnp.max(got[...], axis=0))
    fg_ref[...] = factor[0:1]
    fu_ref[...] = factor[1:2]
    scale = 1.0 / factor

    def here(turn, c):
        owner = ring_row((place + turn) % n, n)
        return pl.ds(pl.multiple_of(owner * rows + c * size, size), size)

    def send(way, step, c, first=False):
        at = here((n - step) if way == 0 else step, c)
        return pltpu.make_async_remote_copy(
            src_ref=narrow.at[way, pl.ds(c * size, size)] if first else outs[way].at[at],
            dst_ref=outs[way].at[at],
            send_sem=send_sem.at[way, step, c],
            recv_sem=recv_sem.at[way, step, c],
            device_id={"rows": to[way]},
            device_id_type=MESH,
        )

    def landed(way, step, c):
        at = here((n - step - 1) if way == 0 else (step + 1), c)
        pltpu.make_async_remote_copy(
            src_ref=outs[way].at[at],
            dst_ref=outs[way].at[at],
            send_sem=send_sem.at[way, step, c],
            recv_sem=recv_sem.at[way, step, c],
            device_id={"rows": to[way]},
            device_id_type=MESH,
        ).wait_recv()

    for c in range(chunks + 1):
        for way in range(2):
            if c < chunks:
                by = jnp.broadcast_to(scale[way : way + 1, :], (16, columns))

                @pl.loop(0, size // 16)
                def _(i):
                    at = pl.ds(pl.multiple_of(c * size + i * 16, 16), 16)
                    narrow[way, at, :] = (fresh[way, at, :] * by).astype(jnp.bfloat16)

            if c:
                send(way, 0, c - 1, True).start()
    own = [
        pltpu.make_async_copy(
            narrow.at[way], outs[way].at[pl.ds(pl.multiple_of(me * rows, rows), rows)], own_sem.at[way]
        )
        for way in range(2)
    ]
    for copy in own:
        copy.start()

    @pl.loop(1, n - 1)
    def _(step):
        for c in range(chunks):
            for way in range(2):
                landed(way, step - 1, c)
                send(way, step, c).start()

    for c in range(chunks):
        for way in range(2):
            landed(way, n - 2, c)

    for copy in own:
        copy.wait()
    for c in range(chunks):
        for way in range(2):
            send(way, 0, c, True).wait_send()

    @pl.loop(1, n - 1)
    def _(step):
        for c in range(chunks):
            for way in range(2):
                send(way, step, c).wait_send()


def serve(w_gate, avg_gate, w_up, avg_up, norm_gain, n):
    rows, columns = w_gate.shape
    chunks = CHUNKS
    while rows % (16 * chunks):
        chunks -= 1
    whole = jax.ShapeDtypeStruct((n * rows, columns), jnp.bfloat16)
    line = jax.ShapeDtypeStruct((1, columns), jnp.float32)
    gain = jnp.broadcast_to(norm_gain[:, None], (rows, 128))
    anywhere = pl.BlockSpec(memory_space=pl.ANY)
    near = pl.BlockSpec(memory_space=pltpu.VMEM)
    return pl.pallas_call(
        functools.partial(serve_kernel, n, chunks),
        out_shape=(whole, whole, line, line),
        in_specs=[near] + [anywhere] * 4,
        out_specs=(anywhere, anywhere, near, near),
        scratch_shapes=[
            pltpu.VMEM((2, rows, columns), jnp.float32),
            pltpu.VMEM((2, rows, columns), jnp.float32),
            pltpu.VMEM((2, rows, columns), jnp.bfloat16),
            pltpu.VMEM((2, columns), jnp.float32),
            pltpu.VMEM((n - 1, 2, columns), jnp.float32),
            pltpu.SemaphoreType.DMA((chunks, 2, 2)),
            pltpu.SemaphoreType.DMA((n - 1,)),
            pltpu.SemaphoreType.DMA((n - 1,)),
            pltpu.SemaphoreType.DMA((2, n - 1, chunks)),
            pltpu.SemaphoreType.DMA((2, n - 1, chunks)),
            pltpu.SemaphoreType.DMA((2,)),
        ],
        compiler_params=pltpu.CompilerParams(
            collective_id=0, has_side_effects=True, vmem_limit_bytes=VMEM_LIMIT
        ),
        name="serve",
    )(gain, w_gate, avg_gate, w_up, avg_up)


def local(n, w_gate, avg_gate, w_up, avg_up, norm_gain):
    serve_gate, serve_up, factor_gate, factor_up = serve(w_gate, avg_gate, w_up, avg_up, norm_gain, n)
    return (serve_gate, serve_up, factor_gate[0], factor_up[0])


def solution(mesh):
    placed = (P("rows", "width"),) * 4 + (P("rows"),)
    return jax.shard_map(
        functools.partial(local, mesh.shape["rows"]),
        mesh=mesh,
        in_specs=placed,
        out_specs=(P(None, "width"), P(None, "width"), P("width"), P("width")),
        check_vma=False,
    )
```

```python
import functools

import jax
import jax.numpy as jnp
from jax import lax
from jax.experimental import pallas as pl
from jax.experimental.pallas import tpu as pltpu
from jax.sharding import PartitionSpec as P

keep_rate = 0.7
MESH = pl.DeviceIdType.MESH
CHUNKS = 4
VMEM_LIMIT = 60 * 2**20


def ring_place(r, n):
    if n % 2:
        return r
    x, z = r % 2, r // 2
    return z + x * (n - 1 - 2 * z)


def ring_row(p, n):
    if n % 2:
        return p
    half = n // 2
    x, k = p // half, p % half
    return 2 * (k + x * (half - 1 - 2 * k)) + x


def serve_kernel(
    n, chunks, gain_ref, wg_ref, ag_ref, wu_ref, au_ref, go_ref, uo_ref, fg_ref, fu_ref,
    w_in, fresh, narrow, gains, part, got, in_sem, max_send, max_recv, send_sem, recv_sem, own_sem,
):
    me = lax.axis_index("rows")
    place = ring_place(me, n)
    nxt = ring_row((place + 1) % n, n)
    prv = ring_row((place + n - 1) % n, n)
    rows, columns = wg_ref.shape
    size = rows // chunks
    outs, to = (go_ref, uo_ref), (nxt, prv)

    loads = []
    for c in range(chunks):
        at = pl.ds(c * size, size)
        for k, (w_ref, avg_ref) in enumerate(((wg_ref, ag_ref), (wu_ref, au_ref))):
            for j, (src, dst) in enumerate(((w_ref, w_in), (avg_ref, fresh))):
                load = pltpu.make_async_copy(src.at[at], dst.at[k, at], in_sem.at[c, k, j])
                load.start()
                loads.append(load)

    barrier = pltpu.get_barrier_semaphore()
    for d in range(1, n):
        pl.semaphore_signal(barrier, inc=1, device_id={"rows": (me + d) % n}, device_id_type=MESH)

    for first in range(0, rows, 128):
        count = min(128, rows - first)
        line = gain_ref[first : first + count].reshape(1, count)
        gains[first : first + count, :] = jnp.broadcast_to(line, (128, count)).T

    tops = [jnp.zeros((8, columns), jnp.float32)] * 2
    for c in range(chunks):
        for k in range(2):
            loads[(c * 2 + k) * 2].wait()
            loads[(c * 2 + k) * 2 + 1].wait()

            def blend(i, top):
                at = pl.ds(pl.multiple_of(c * size + i * 8, 8), 8)
                gain = jnp.tile(gains[at, :], (1, columns // 128))
                value = (keep_rate * fresh[k, at, :] + (1.0 - keep_rate) * w_in[k, at, :]) * gain
                fresh[k, at, :] = value
                return jnp.maximum(top, jnp.abs(value))

            tops[k] = lax.fori_loop(0, size // 8, blend, tops[k])
    for k in range(2):
        part[k : k + 1, :] = jnp.max(tops[k], axis=0, keepdims=True)

    pl.semaphore_wait(barrier, n - 1)
    copies = []
    for d in range(1, n):
        copy = pltpu.make_async_remote_copy(
            src_ref=part,
            dst_ref=got.at[d - 1],
            send_sem=max_send.at[d - 1],
            recv_sem=max_recv.at[d - 1],
            device_id={"rows": (me + d) % n},
            device_id_type=MESH,
        )
        copy.start()
        copies.append(copy)
    for copy in copies:
        copy.wait()
    factor = jnp.maximum(part[...], jnp.max(got[...], axis=0))
    fg_ref[...] = factor[0:1]
    fu_ref[...] = factor[1:2]
    scale = 1.0 / factor

    def here(turn, c):
        owner = ring_row((place + turn) % n, n)
        return pl.ds(pl.multiple_of(owner * rows + c * size, size), size)

    def send(way, step, c, first=False):
        at = here((n - step) if way == 0 else step, c)
        return pltpu.make_async_remote_copy(
            src_ref=narrow.at[way, pl.ds(c * size, size)] if first else outs[way].at[at],
            dst_ref=outs[way].at[at],
            send_sem=send_sem.at[way, step, c],
            recv_sem=recv_sem.at[way, step, c],
            device_id={"rows": to[way]},
            device_id_type=MESH,
        )

    def landed(way, step, c):
        at = here((n - step - 1) if way == 0 else (step + 1), c)
        pltpu.make_async_remote_copy(
            src_ref=outs[way].at[at],
            dst_ref=outs[way].at[at],
            send_sem=send_sem.at[way, step, c],
            recv_sem=recv_sem.at[way, step, c],
            device_id={"rows": to[way]},
            device_id_type=MESH,
        ).wait_recv()

    for c in range(chunks + 1):
        for way in range(2):
            if c < chunks:
                by = jnp.broadcast_to(scale[way : way + 1, :], (16, columns))

                @pl.loop(0, size // 16)
                def _(i):
                    at = pl.ds(pl.multiple_of(c * size + i * 16, 16), 16)
                    narrow[way, at, :] = (fresh[way, at, :] * by).astype(jnp.bfloat16)

            if c:
                send(way, 0, c - 1, True).start()
    own = [
        pltpu.make_async_copy(
            narrow.at[way], outs[way].at[pl.ds(pl.multiple_of(me * rows, rows), rows)], own_sem.at[way]
        )
        for way in range(2)
    ]
    for copy in own:
        copy.start()

    @pl.loop(1, n - 1)
    def _(step):
        for c in range(chunks):
            for way in range(2):
                landed(way, step - 1, c)
                send(way, step, c).start()

    for c in range(chunks):
        for way in range(2):
            landed(way, n - 2, c)

    for copy in own:
        copy.wait()
    for c in range(chunks):
        for way in range(2):
            send(way, 0, c, True).wait_send()

    @pl.loop(1, n - 1)
    def _(step):
        for c in range(chunks):
            for way in range(2):
                send(way, step, c).wait_send()


def serve(w_gate, avg_gate, w_up, avg_up, norm_gain, n):
    rows, columns = w_gate.shape
    chunks = CHUNKS
    while rows % (16 * chunks):
        chunks -= 1
    whole = jax.ShapeDtypeStruct((n * rows, columns), jnp.bfloat16)
    line = jax.ShapeDtypeStruct((1, columns), jnp.float32)
    anywhere = pl.BlockSpec(memory_space=pl.ANY)
    near = pl.BlockSpec(memory_space=pltpu.VMEM)
    return pl.pallas_call(
        functools.partial(serve_kernel, n, chunks),
        out_shape=(whole, whole, line, line),
        in_specs=[near] + [anywhere] * 4,
        out_specs=(anywhere, anywhere, near, near),
        scratch_shapes=[
            pltpu.VMEM((2, rows, columns), jnp.float32),
            pltpu.VMEM((2, rows, columns), jnp.float32),
            pltpu.VMEM((2, rows, columns), jnp.bfloat16),
            pltpu.VMEM((rows, 128), jnp.float32),
            pltpu.VMEM((2, columns), jnp.float32),
            pltpu.VMEM((n - 1, 2, columns), jnp.float32),
            pltpu.SemaphoreType.DMA((chunks, 2, 2)),
            pltpu.SemaphoreType.DMA((n - 1,)),
            pltpu.SemaphoreType.DMA((n - 1,)),
            pltpu.SemaphoreType.DMA((2, n - 1, chunks)),
            pltpu.SemaphoreType.DMA((2, n - 1, chunks)),
            pltpu.SemaphoreType.DMA((2,)),
        ],
        compiler_params=pltpu.CompilerParams(
            collective_id=0, has_side_effects=True, vmem_limit_bytes=VMEM_LIMIT
        ),
        name="serve",
    )(norm_gain, w_gate, avg_gate, w_up, avg_up)


def local(n, w_gate, avg_gate, w_up, avg_up, norm_gain):
    serve_gate, serve_up, factor_gate, factor_up = serve(w_gate, avg_gate, w_up, avg_up, norm_gain, n)
    return (serve_gate, serve_up, factor_gate[0], factor_up[0])


def solution(mesh):
    placed = (P("rows", "width"),) * 4 + (P("rows"),)
    return jax.shard_map(
        functools.partial(local, mesh.shape["rows"]),
        mesh=mesh,
        in_specs=placed,
        out_specs=(P(None, "width"), P(None, "width"), P("width"), P("width")),
        check_vma=False,
    )
```
